512 devices in a mesh: gx: 16 (over x, z_lo), gy: 16 (over y, core), af: 2 (over z_hi).
Axes of the slice: x: 4, y: 8, z: 8 (z_hi: 2, z_lo: 4; z = z_hi * 4 + z_lo), core: 2. Of those that a mesh axis runs over, the one named last changes fastest.
Arguments:
- points: bfloat16 [16384, 256], P(('gx', 'gy'), 'af'), may hold values from -12 to 12
- targets: float32 [16384, 16], P(('gx', 'gy')), may hold values from -6 to 6
Outputs:
- solution: float32 [16384, 16], P(('gx', 'gy'))
- residual: float32 [16384, 16], P(('gx', 'gy'))
The draws below stay inside these ranges and needn't reach their ends.
All inputs are finite; a program needn't handle non-finite values.
Results may differ from the reference program's by a relative error of at most 0.025.
Values may be sent and summed in bfloat16 or wider, within the bound.
A program may use at most 64 MiB of HBM per device.

```python
import jax
import jax.numpy as jnp
from jax import lax

F = 256
R = 16
P_DEV = 64
ITERS = 2
N_PTS = 16384


def draw_points(key, part):
    keys = jax.random.split(jax.random.fold_in(key, 11), 5)
    labels = jax.random.randint(keys[0], (N_PTS,), 0, 16)
    one_hot = (labels[:, None] == jnp.arange(16, dtype=jnp.int32)[None, :]).astype(jnp.float32)
    centres = 1.4 * jax.random.normal(keys[1], (16, F), jnp.float32)
    spread = jnp.exp(jax.random.uniform(keys[3], (16,), jnp.float32, 0.0, 0.47))
    noise = jax.random.normal(keys[4], (N_PTS, F), jnp.float32)
    row_centres = jnp.dot(one_hot, centres, precision=lax.Precision.HIGHEST)
    row_spread = jnp.dot(one_hot, spread, precision=lax.Precision.HIGHEST)
    values = row_centres + row_spread[:, None] * noise
    return jnp.clip(values, -12.0, 12.0).astype(jnp.bfloat16)


def block_scale(own_key, extent, pieces, smallest, high):
    factor_of, own = 1.0, jax.random.fold_in(own_key, 6)
    for dim, shards_of in pieces:
        draws = jnp.exp(jax.random.uniform(jax.random.fold_in(own, dim), (shards_of,), jnp.float32, smallest / len(pieces), high / len(pieces)))
        factor_of = factor_of * jnp.repeat(draws, extent[dim] // shards_of).reshape([-1 if axis == dim else 1 for axis in range(len(extent))])
    return factor_of


def bell_draw(own_key, dims, scale, bound, pieces=(), kind=jnp.bfloat16):
    drawn = jax.random.normal(own_key, dims, jnp.float32) * scale
    if len(pieces) > 0:
        drawn = block_scale(own_key, dims, pieces, -0.22, 0.18) * drawn
    return jnp.clip(drawn, min=-bound, max=bound).astype(kind)


def setup_inputs(seed: int = 0) -> dict:
    streams_of = jax.random.split(jax.random.key(seed), 3)
    points = draw_points(jax.random.fold_in(streams_of[2], 71), 0)
    targets = bell_draw(streams_of[1], (N_PTS, R), 1.0, 6.0, ((0, 256),), jnp.float32)
    return dict(points=points, targets=targets)


def operate(coords, norms, vector):
    lowered = lax.optimization_barrier(vector.astype(jnp.bfloat16)).astype(jnp.float32)
    scale = 0.5 / F
    blocks = coords.reshape(N_PTS // P_DEV, P_DEV, F)
    block_norms = norms.reshape(N_PTS // P_DEV, P_DEV)

    def one_block(pair):
        rows, row_norms = pair
        inner = jnp.dot(rows, coords.T)
        distance = row_norms[:, None] + norms[None, :] - 2.0 * inner
        kernel = lax.optimization_barrier(jnp.exp(-scale * distance).astype(jnp.bfloat16)).astype(jnp.float32)
        return jnp.dot(kernel, lowered)

    product = lax.map(one_block, (blocks, block_norms)).reshape(N_PTS, R)
    return product + 0.1 * vector


def reference(points, targets):
    coords = points.astype(jnp.float32)
    norms = jnp.sum(coords * coords, axis=1)
    solution = jnp.zeros_like(targets)
    residual = targets
    direction = targets
    norm_now = jnp.sum(residual * residual, axis=0)
    for step in range(ITERS):
        image = operate(coords, norms, direction)
        alpha = norm_now / jnp.sum(direction * image, axis=0)
        solution = solution + alpha * direction
        residual = residual - alpha * image
        norm_next = jnp.sum(residual * residual, axis=0)
        direction = residual + (norm_next / norm_now) * direction
        norm_now = norm_next
    return solution, residual
```

```python
import math

import jax
import jax.numpy as jnp
from jax import lax
from jax.experimental import pallas as pl
from jax.experimental.pallas import tpu as pltpu
from jax.sharding import Mesh
from jax.sharding import PartitionSpec as P

AXES = ("gx_0", "gx_1", "gy_0", "gy_1", "af")
GX_GY = ("gx_0", "gx_1", "gy_0", "gy_1")
MESH = pl.DeviceIdType.MESH
X, ZL, Y, C, ZH = 4, 4, 8, 2, 2
Z = ZL * ZH
NXZ, NY = X * Z, Y * C
HALF, F, R = 32, 256, 16
F32, BF16 = jnp.float32, jnp.bfloat16


def swap_blocks(tile):
    rows = lax.broadcasted_iota(jnp.int32, (16, 128), 0) // 4
    lanes = lax.broadcasted_iota(jnp.int32, (16, 128), 1) // 32
    shift = (rows - lanes) & 3
    out = tile
    for d in range(1, 4):
        moved = pltpu.roll(pltpu.roll(tile, 128 - 32 * d, 1), 4 * d, 0)
        out = jnp.where(shift == d, moved, out)
    return out


def group_sums(packed):
    group = lax.broadcasted_iota(jnp.int32, (4, 128), 1) // 32
    spread = jnp.concatenate([jnp.where(group == g, packed, 0.0) for g in range(4)], axis=0)
    sums = jnp.sum(spread, axis=1, keepdims=True)
    out = jnp.broadcast_to(sums[12:16], (4, 128))
    for g in range(3):
        out = jnp.where(group == g, sums[4 * g : 4 * g + 4], out)
    return out


def low_lanes():
    return (lax.broadcasted_iota(jnp.int32, (4, 128), 1) & 31) < 16


def paired(first, second):
    return jnp.where(low_lanes(), first, second)


def unpaired(both):
    low = low_lanes()
    return (
        jnp.where(low, both, pltpu.roll(both, 16, 1)),
        jnp.where(low, pltpu.roll(both, 112, 1), both),
    )


def tree_sum(terms):
    while len(terms) > 1:
        terms = [sum(terms[i : i + 2][1:], terms[i]) for i in range(0, len(terms), 2)]
    return terms[0]


def kernel(
    points, targets, solution_ref, residual_ref,
    cols, rows, kmat, vb, vw, vu, bi, wi, ys1, yr1, ys2, yr2, square, send, recv,
):
    x, zl, y, c, zh = (lax.axis_index(a) for a in AXES)
    z = zh * ZL + zl
    me = (x * ZL + zl) * ZH + zh
    mine = y * C + c
    own = (x * ZL + zl) * ZH

    def z_peers():
        for d in (4, 3, 5, 2, 6, 1, 7):
            other = (z + d) % Z
            yield (x, other % ZL, y, c, other // ZL)

    def x_peers():
        for d in (2, 1, 3):
            yield ((x + d) % X, zl, y, c, zh)

    def xz_peers():
        for dz in (4, 3, 5, 2, 6, 1, 7, 0):
            for dx in (2, 1, 3, 0):
                if dz or dx:
                    other = (z + dz) % Z
                    yield ((x + dx) % X, other % ZL, y, c, other // ZL)

    def y_peers():
        for d in (4, 3, 5, 2, 6, 1, 7, 0):
            for e in (1, 0):
                if d or e:
                    yield (x, zl, (y + d) % Y, (c + e) % C, zh)

    def push(src, dst, stage, device):
        pltpu.make_async_remote_copy(
            src_ref=src, dst_ref=dst, send_sem=send.at[stage], recv_sem=recv.at[stage],
            device_id=device, device_id_type=MESH,
        ).start()

    def arrived(ref, stage):
        pltpu.make_async_copy(ref, ref, recv.at[stage]).wait()

    def sent(ref, stage):
        pltpu.make_async_copy(ref, ref, send.at[stage]).wait()

    barrier = pltpu.get_barrier_semaphore()
    greeted = 0
    for peers in (z_peers, x_peers, y_peers):
        for device in peers():
            pl.semaphore_signal(barrier, inc=1, device_id=device, device_id_type=MESH)
            greeted += 1

    square[...] = jnp.zeros_like(square)
    square[0:64, 0:R] = targets[...]
    halves = swap_blocks(jnp.transpose(square[...])[0:16])
    b_own = jnp.where(zh == 0, halves[0:4], halves[4:8])
    vb[me] = jnp.concatenate([b_own, b_own], axis=0)
    bi[mine] = jnp.concatenate([b_own, b_own], axis=0)
    cols[zh, x, zl] = points[...]
    pl.semaphore_wait(barrier, greeted)

    for device in z_peers():
        push(points, cols.at[zh, x, zl], 0, device)
        push(vb.at[me], vb.at[me], 1, device)
    for device in y_peers():
        push(vb.at[me], bi.at[mine], 2, device)
    arrived(rows.at[:, 0:7], 0)
    arrived(vb.at[0:7], 1)

    for device in x_peers():
        push(cols.at[:, x], cols.at[:, x], 3, device)
        push(vb.at[pl.ds(x * Z, Z)], vb.at[pl.ds(x * Z, Z)], 4, device)
    for device in y_peers():
        push(cols.at[:, x, zl, zh], rows.at[:, mine], 5, device)
    rows[:, mine] = cols[:, x, zl, zh]
    arrived(rows.at[:, 0:15], 5)

    scale = 0.5 / F * math.log2(math.e)
    row_points = jnp.concatenate(
        [rows[0].reshape(NY * HALF, 128), rows[1].reshape(NY * HALF, 128)], axis=1
    )
    wide = row_points.astype(F32)
    squares = wide * wide
    high = squares.astype(BF16)
    low = (squares - high.astype(F32)).astype(BF16)
    ones = jnp.ones((8, F), BF16)
    contract = (((1,), (1,)), ((), ()))
    row_norms = (
        lax.dot_general(ones, high, contract, preferred_element_type=F32)
        + lax.dot_general(ones, low, contract, preferred_element_type=F32)
    )[0:1] * scale

    arrived(cols.at[:, 0:3], 3)
    arrived(vb.at[0:24], 4)
    for part in range(X):
        col_points = jnp.concatenate(
            [cols[0, part].reshape(256, 128), cols[1, part].reshape(256, 128)], axis=1
        )
        wide = col_points.astype(F32)
        col_norms = jnp.sum(wide * wide, axis=1, keepdims=True) * scale
        inner = lax.dot_general(col_points, row_points, contract, preferred_element_type=F32)
        kmat[pl.ds(part * 256, 256)] = jnp.exp2(
            (2.0 * scale) * inner - (row_norms + col_norms)
        ).astype(BF16)

    def partial_product(slots):
        wide = [
            swap_blocks(jnp.concatenate(slots[4 * j : 4 * j + 4], axis=0)).astype(BF16)
            for j in range(NXZ // 4)
        ]
        vector = jnp.concatenate(wide, axis=1)
        return jnp.dot(vector, kmat[...], preferred_element_type=F32)

    def to_owners(product, weights, ys, yr, stage):
        blocks = []
        for j in range(NY // 4):
            block = swap_blocks(product[:, 128 * j : 128 * j + 128])
            blocks += [block[4 * s : 4 * s + 4] for s in range(4)]
        share = group_sums(tree_sum([w * b for w, b in zip(weights, blocks)]))
        for t in range(NY):
            ys[t] = jnp.concatenate([blocks[t], share], axis=0)
        for device in y_peers():
            push(ys.at[device[2] * C + device[3]], yr.at[mine], stage, device)
        yr[mine] = ys[mine]
        arrived(yr.at[0:15], stage)
        return tree_sum([yr[t] for t in range(NY)])

    arrived(bi.at[0:15], 2)
    b_rows = [bi[t, 0:4] for t in range(NY)]
    b_cols = [vb[s, 0:4] for s in range(NXZ)]
    total = to_owners(partial_product(b_cols), b_rows, ys1, yr1, 6)
    bb_here = group_sums(tree_sum([b * b for b in b_rows]))
    w_own = total[0:4] + 0.1 * b_own
    vw[me] = jnp.concatenate([w_own, paired(total[4:8], bb_here)], axis=0)
    wi[mine] = jnp.concatenate([w_own, w_own], axis=0)
    for device in xz_peers():
        push(vw.at[me], vw.at[me], 7, device)
    for device in y_peers():
        push(vw.at[me], wi.at[mine], 8, device)
    arrived(vw.at[0:31], 7)
    bkb, bb = unpaired(tree_sum([vw[s, 4:8] for s in range(NXZ)]))
    alpha = bb / (bkb + 0.1 * bb)

    r_cols = [b_cols[s] - alpha * vw[s, 0:4] for s in range(NXZ)]
    product = partial_product(r_cols)
    arrived(wi.at[0:15], 8)
    r_rows = [b_rows[t] - alpha * wi[t, 0:4] for t in range(NY)]
    rr_here = group_sums(tree_sum([r * r for r in r_rows]))
    total = to_owners(product, r_rows, ys2, yr2, 9)
    r_own = b_own - alpha * w_own
    u_own = total[0:4] + 0.1 * r_own
    vu[me] = jnp.concatenate([u_own, paired(total[4:8], rr_here)], axis=0)
    for device in xz_peers():
        push(vu.at[me], vu.at[me], 10, device)
    arrived(vu.at[0:31], 10)
    rkr, rr = unpaired(tree_sum([vu[s, 4:8] for s in range(NXZ)]))
    ratio = rr / bb
    alpha_next = rr / (rkr + 0.1 * rr - ratio * rr / alpha)

    def result(halves, out):
        packed = jnp.concatenate([*halves, jnp.zeros((8, 128), F32)], axis=0)
        square[0:16, :] = swap_blocks(packed)
        out[...] = jnp.transpose(square[...])[0:64, 0:R]

    solutions, residuals = [], []
    for h in range(2):
        b, w, u = vb[own + h, 0:4], vw[own + h, 0:4], vu[own + h, 0:4]
        r = b - alpha * w
        solutions.append(alpha * b + alpha_next * (r + ratio * b))
        residuals.append(r - alpha_next * (u + ratio * w))
    result(solutions, solution_ref)
    result(residuals, residual_ref)

    sent(rows.at[:, 0:7], 0)
    sent(vb.at[0:7], 1)
    sent(bi.at[0:15], 2)
    sent(cols.at[:, 0:3], 3)
    sent(vb.at[0:24], 4)
    sent(rows.at[:, 0:15], 5)
    sent(yr1.at[0:15], 6)
    sent(vw.at[0:31], 7)
    sent(wi.at[0:15], 8)
    sent(yr2.at[0:15], 9)
    sent(vu.at[0:31], 10)


def local(points, targets):
    vmem = pl.BlockSpec(memory_space=pltpu.VMEM)
    message = lambda n: pltpu.VMEM((n, 8, 128), F32)
    return pl.pallas_call(
        kernel,
        out_shape=[jax.ShapeDtypeStruct(targets.shape, F32)] * 2,
        in_specs=[vmem, vmem],
        out_specs=[vmem, vmem],
        scratch_shapes=[
            pltpu.VMEM((2, X, ZL, ZH, HALF, 128), BF16),
            pltpu.VMEM((2, NY, HALF, 128), BF16),
            pltpu.VMEM((NXZ * HALF, NY * HALF), BF16),
            message(NXZ), message(NXZ), message(NXZ),
            message(NY), message(NY),
            message(NY), message(NY), message(NY), message(NY),
            pltpu.VMEM((128, 128), F32),
            pltpu.SemaphoreType.DMA((11,)),
            pltpu.SemaphoreType.DMA((11,)),
        ],
        compiler_params=pltpu.CompilerParams(collective_id=0, has_side_effects=True),
    )(points.reshape(2, HALF, 128), targets)


def solution(mesh):
    torus = Mesh(mesh.devices.reshape(X, ZL, Y, C, ZH), AXES)
    in_specs = (P(GX_GY, "af"), P(GX_GY, None))
    out_specs = (P(GX_GY, None), P(GX_GY, None))
    return jax.shard_map(local, mesh=torus, in_specs=in_specs, out_specs=out_specs, check_vma=False)
```

```python
import math

import jax
import jax.numpy as jnp
from jax import lax
from jax.experimental import pallas as pl
from jax.experimental.pallas import tpu as pltpu
from jax.sharding import Mesh
from jax.sharding import PartitionSpec as P

AXES = ("gx_0", "gx_1", "gy_0", "gy_1", "af")
GX_GY = ("gx_0", "gx_1", "gy_0", "gy_1")
MESH = pl.DeviceIdType.MESH
X, ZL, Y, C, ZH = 4, 4, 8, 2, 2
Z = ZL * ZH
NXZ, NY = X * Z, Y * C
HALF, F, R = 32, 256, 16
F32, BF16 = jnp.float32, jnp.bfloat16


def swap_blocks(tile):
    rows = lax.broadcasted_iota(jnp.int32, (16, 128), 0) // 4
    lanes = lax.broadcasted_iota(jnp.int32, (16, 128), 1) // 32
    shift = (rows - lanes) & 3
    out = tile
    for d in range(1, 4):
        moved = pltpu.roll(pltpu.roll(tile, 128 - 32 * d, 1), 4 * d, 0)
        out = jnp.where(shift == d, moved, out)
    return out


def group_sums(packed):
    group = lax.broadcasted_iota(jnp.int32, (4, 128), 1) // 32
    spread = jnp.concatenate([jnp.where(group == g, packed, 0.0) for g in range(4)], axis=0)
    sums = jnp.sum(spread, axis=1, keepdims=True)
    out = jnp.broadcast_to(sums[12:16], (4, 128))
    for g in range(3):
        out = jnp.where(group == g, sums[4 * g : 4 * g + 4], out)
    return out


def low_lanes():
    return (lax.broadcasted_iota(jnp.int32, (4, 128), 1) & 31) < 16


def paired(first, second):
    return jnp.where(low_lanes(), first, second)


def unpaired(both):
    low = low_lanes()
    return (
        jnp.where(low, both, pltpu.roll(both, 16, 1)),
        jnp.where(low, pltpu.roll(both, 112, 1), both),
    )


def tree_sum(terms):
    while len(terms) > 1:
        terms = [sum(terms[i : i + 2][1:], terms[i]) for i in range(0, len(terms), 2)]
    return terms[0]


def kernel(
    points, targets, solution_ref, residual_ref,
    cols, rows, kmat, vb, vw, vu, bi, wi, ys1, yr1, ys2, yr2, send, recv,
):
    x, zl, y, c, zh = (lax.axis_index(a) for a in AXES)
    z = zh * ZL + zl
    me = (x * ZL + zl) * ZH + zh
    mine = y * C + c
    own = (x * ZL + zl) * ZH

    def z_peers():
        for d in (4, 3, 5, 2, 6, 1, 7):
            other = (z + d) % Z
            yield (x, other % ZL, y, c, other // ZL)

    def x_peers():
        for d in (2, 1, 3):
            yield ((x + d) % X, zl, y, c, zh)

    def xz_peers():
        for dz in (4, 3, 5, 2, 6, 1, 7, 0):
            for dx in (2, 1, 3, 0):
                if dz or dx:
                    other = (z + dz) % Z
                    yield ((x + dx) % X, other % ZL, y, c, other // ZL)

    def y_peers():
        for d in (4, 3, 5, 2, 6, 1, 7, 0):
            for e in (1, 0):
                if d or e:
                    yield (x, zl, (y + d) % Y, (c + e) % C, zh)

    def push(src, dst, stage, device):
        pltpu.make_async_remote_copy(
            src_ref=src, dst_ref=dst, send_sem=send.at[stage], recv_sem=recv.at[stage],
            device_id=device, device_id_type=MESH,
        ).start()

    pending = []

    def arrived(ref, stage):
        pltpu.make_async_copy(ref, ref, recv.at[stage]).wait()
        pending.append((ref, stage))

    def sent(ref, stage):
        pltpu.make_async_copy(ref, ref, send.at[stage]).wait()

    barrier = pltpu.get_barrier_semaphore()
    greeted = 0
    for peers in (z_peers, x_peers, y_peers):
        for device in peers():
            pl.semaphore_signal(barrier, inc=1, device_id=device, device_id_type=MESH)
            greeted += 1

    halves = swap_blocks(jnp.concatenate([targets[...], targets[...]], axis=1))
    b_own = jnp.where(zh == 0, halves[0:4], halves[4:8])
    vb[me] = b_own
    bi[mine] = b_own
    cols[zh, x, zl] = points[...]
    pl.semaphore_wait(barrier, greeted)

    def z_at(d):
        other = (z + d) % Z
        return other // ZL, other % ZL

    def along_x(zh_of, zl_of):
        block = cols.at[zh_of, x, zl_of]
        for device in x_peers():
            push(block, block, 3, device)

    for d in (4, 3, 5, 2, 6, 1, 7):
        zh_of, zl_of = z_at(d)
        push(points, cols.at[zh, x, zl], 11 + (Z - d), (x, zl_of, y, c, zh_of))
    for device in x_peers():
        push(points, cols.at[zh, x, zl], 3, device)
    for device in z_peers():
        push(vb.at[me], vb.at[me], 1, device)
    for device in y_peers():
        push(points.at[zh], rows.at[zh, mine], 5, device)
    for device in y_peers():
        push(vb.at[me], bi.at[mine], 2, device)
    rows[zh, mine] = points[zh]
    for d in (1, 7, 2, 6, 3, 5):
        arrived(rows.at[:, 0], 11 + d)
        along_x(*z_at(d))
    arrived(rows.at[:, 0], 11 + 4)
    for device in y_peers():
        push(cols.at[1 - zh, x, zl, zh], rows.at[1 - zh, mine], 5, device)
    along_x(1 - zh, zl)
    rows[1 - zh, mine] = cols[1 - zh, x, zl, zh]
    arrived(vb.at[0:7], 1)
    for device in x_peers():
        push(vb.at[pl.ds(x * Z, Z)], vb.at[pl.ds(x * Z, Z)], 4, device)
    arrived(rows.at[:, 0:15], 5)

    scale = 0.5 / F * math.log2(math.e)
    row_points = jnp.concatenate(
        [rows[0].reshape(NY * HALF, 128), rows[1].reshape(NY * HALF, 128)], axis=1
    )
    wide = row_points.astype(F32)
    squares = wide * wide
    high = squares.astype(BF16)
    low = (squares - high.astype(F32)).astype(BF16)
    ones = jnp.ones((8, F), BF16)
    contract = (((1,), (1,)), ((), ()))
    row_norms = (
        lax.dot_general(ones, high, contract, preferred_element_type=F32)
        + lax.dot_general(ones, low, contract, preferred_element_type=F32)
    )[0:1] * scale

    arrived(cols.at[:, 0:3], 3)
    arrived(vb.at[0:24], 4)
    for part in range(X):
        col_points = jnp.concatenate(
            [cols[0, part].reshape(256, 128), cols[1, part].reshape(256, 128)], axis=1
        )
        wide = col_points.astype(F32)
        col_norms = jnp.sum(wide * wide, axis=1, keepdims=True) * scale
        inner = lax.dot_general(col_points, row_points, contract, preferred_element_type=F32)
        kmat[pl.ds(part * 256, 256)] = jnp.exp2(
            (2.0 * scale) * inner - (row_norms + col_norms)
        ).astype(BF16)

    def partial_product(slots):
        wide = [
            swap_blocks(jnp.concatenate(slots[4 * j : 4 * j + 4], axis=0)).astype(BF16)
            for j in range(NXZ // 4)
        ]
        vector = jnp.concatenate(wide, axis=1)
        return jnp.dot(vector, kmat[...], preferred_element_type=F32)

    def to_owners(product, weights, ys, yr, stage):
        blocks = []
        for j in range(NY // 4):
            block = swap_blocks(product[:, 128 * j : 128 * j + 128])
            blocks += [block[4 * s : 4 * s + 4] for s in range(4)]
        share = group_sums(tree_sum([w * b for w, b in zip(weights, blocks)]))
        for t in range(NY):
            ys[t] = jnp.concatenate([blocks[t], share], axis=0)
        for device in y_peers():
            push(ys.at[device[2] * C + device[3]], yr.at[mine], stage, device)
        yr[mine] = ys[mine]
        arrived(yr.at[0:15], stage)
        return tree_sum([yr[t] for t in range(NY)])

    arrived(bi.at[0:15], 2)
    b_rows = [bi[t] for t in range(NY)]
    b_cols = [vb[s] for s in range(NXZ)]
    total = to_owners(partial_product(b_cols), b_rows, ys1, yr1, 6)
    bb_here = group_sums(tree_sum([b * b for b in b_rows]))
    w_own = total[0:4] + 0.1 * b_own
    vw[me] = jnp.concatenate([w_own, paired(total[4:8], bb_here)], axis=0)
    wi[mine] = w_own
    for device in xz_peers():
        push(vw.at[me], vw.at[me], 7, device)
    for device in y_peers():
        push(wi.at[mine], wi.at[mine], 8, device)
    arrived(vw.at[0:31], 7)
    bkb, bb = unpaired(tree_sum([vw[s, 4:8] for s in range(NXZ)]))
    alpha = bb / (bkb + 0.1 * bb)

    r_cols = [b_cols[s] - alpha * vw[s, 0:4] for s in range(NXZ)]
    product = partial_product(r_cols)
    arrived(wi.at[0:15], 8)
    r_rows = [b_rows[t] - alpha * wi[t] for t in range(NY)]
    rr_here = group_sums(tree_sum([r * r for r in r_rows]))
    total = to_owners(product, r_rows, ys2, yr2, 9)
    r_own = b_own - alpha * w_own
    u_own = total[0:4] + 0.1 * r_own
    vu[me] = jnp.concatenate([u_own, paired(total[4:8], rr_here)], axis=0)
    for device in xz_peers():
        push(vu.at[me], vu.at[me], 10, device)
    arrived(vu.at[0:31], 10)
    rkr, rr = unpaired(tree_sum([vu[s, 4:8] for s in range(NXZ)]))
    ratio = rr / bb
    alpha_next = rr / (rkr + 0.1 * rr - ratio * rr / alpha)

    def result(halves, out):
        packed = jnp.concatenate([*halves, jnp.zeros((8, 128), F32)], axis=0)
        out[...] = swap_blocks(packed)[:, 0:64]

    solutions, residuals = [], []
    for h in range(2):
        b, w, u = vb[own + h], vw[own + h, 0:4], vu[own + h, 0:4]
        r = b - alpha * w
        solutions.append(alpha * b + alpha_next * (r + ratio * b))
        residuals.append(r - alpha_next * (u + ratio * w))
    result(solutions, solution_ref)
    result(residuals, residual_ref)

    for ref, stage in pending:
        sent(ref, stage)


def local(points, targets):
    vmem = pl.BlockSpec(memory_space=pltpu.VMEM)
    message = lambda n, rows=8: pltpu.VMEM((n, rows, 128), F32)
    turned = targets.T
    results = pl.pallas_call(
        kernel,
        out_shape=[jax.ShapeDtypeStruct(turned.shape, F32)] * 2,
        in_specs=[vmem, vmem],
        out_specs=[vmem, vmem],
        scratch_shapes=[
            pltpu.VMEM((2, X, ZL, ZH, HALF, 128), BF16),
            pltpu.VMEM((2, NY, HALF, 128), BF16),
            pltpu.VMEM((NXZ * HALF, NY * HALF), BF16),
            message(NXZ, 4), message(NXZ), message(NXZ),
            message(NY, 4), message(NY, 4),
            message(NY), message(NY), message(NY), message(NY),
            pltpu.SemaphoreType.DMA((19,)),
            pltpu.SemaphoreType.DMA((19,)),
        ],
        compiler_params=pltpu.CompilerParams(collective_id=0, has_side_effects=True),
    )(points.reshape(2, HALF, 128), turned)
    return tuple(result.T for result in results)


def solution(mesh):
    torus = Mesh(mesh.devices.reshape(X, ZL, Y, C, ZH), AXES)
    in_specs = (P(GX_GY, "af"), P(GX_GY, None))
    out_specs = (P(GX_GY, None), P(GX_GY, None))
    return jax.shard_map(local, mesh=torus, in_specs=in_specs, out_specs=out_specs, check_vma=False)
```

```python
import math

import jax
import jax.numpy as jnp
from jax import lax
from jax.experimental import pallas as pl
from jax.experimental.pallas import tpu as pltpu
from jax.sharding import Mesh
from jax.sharding import PartitionSpec as P

AXES = ("gx_0", "gx_1", "gy_0", "gy_1", "af")
GX_GY = ("gx_0", "gx_1", "gy_0", "gy_1")
MESH = pl.DeviceIdType.MESH
X, ZL, Y, C, ZH = 4, 4, 8, 2, 2
Z = ZL * ZH
NXZ, NY = X * Z, Y * C
HALF, F, R = 32, 256, 16
F32, BF16 = jnp.float32, jnp.bfloat16


def swap_blocks(tile):
    rows = lax.broadcasted_iota(jnp.int32, (16, 128), 0) // 4
    lanes = lax.broadcasted_iota(jnp.int32, (16, 128), 1) // 32
    shift = (rows - lanes) & 3
    out = tile
    for d in range(1, 4):
        moved = pltpu.roll(pltpu.roll(tile, 128 - 32 * d, 1), 4 * d, 0)
        out = jnp.where(shift == d, moved, out)
    return out


def group_sums(packed):
    group = lax.broadcasted_iota(jnp.int32, (4, 128), 1) // 32
    spread = jnp.concatenate([jnp.where(group == g, packed, 0.0) for g in range(4)], axis=0)
    sums = jnp.sum(spread, axis=1, keepdims=True)
    out = jnp.broadcast_to(sums[12:16], (4, 128))
    for g in range(3):
        out = jnp.where(group == g, sums[4 * g : 4 * g + 4], out)
    return out


def low_lanes():
    return (lax.broadcasted_iota(jnp.int32, (4, 128), 1) & 31) < 16


def paired(first, second):
    return jnp.where(low_lanes(), first, second)


def unpaired(both):
    low = low_lanes()
    return (
        jnp.where(low, both, pltpu.roll(both, 16, 1)),
        jnp.where(low, pltpu.roll(both, 112, 1), both),
    )


def tree_sum(terms):
    while len(terms) > 1:
        terms = [sum(terms[i : i + 2][1:], terms[i]) for i in range(0, len(terms), 2)]
    return terms[0]


def kernel(
    points, targets, results,
    turned, cols, rows, kmat, vb, vw, vu, sums, bi, wi, ys1, yr1, ys2, yr2, load, send, recv,
):
    x, zl, y, c, zh = (lax.axis_index(a) for a in AXES)
    z = zh * ZL + zl
    me = (x * ZL + zl) * ZH + zh
    mine = y * C + c
    own = (x * ZL + zl) * ZH

    def z_peers():
        for d in (4, 3, 5, 2, 6, 1, 7):
            other = (z + d) % Z
            yield (x, other % ZL, y, c, other // ZL)

    def x_peers():
        for d in (2, 1, 3):
            yield ((x + d) % X, zl, y, c, zh)

    def xz_peers():
        for dz in (4, 3, 5, 2, 6, 1, 7, 0):
            for dx in (2, 1, 3, 0):
                if dz or dx:
                    other = (z + dz) % Z
                    yield ((x + dx) % X, other % ZL, y, c, other // ZL)

    def y_peers():
        for d in (4, 3, 5, 2, 6, 1, 7, 0):
            for e in (1, 0):
                if d or e:
                    yield (x, zl, (y + d) % Y, (c + e) % C, zh)

    def push(src, dst, stage, device):
        pltpu.make_async_remote_copy(
            src_ref=src, dst_ref=dst, send_sem=send.at[stage], recv_sem=recv.at[stage],
            device_id=device, device_id_type=MESH,
        ).start()

    pending = []

    def arrived(ref, stage):
        pltpu.make_async_copy(ref, ref, recv.at[stage]).wait()
        pending.append((ref, stage))

    def sent(ref, stage):
        pltpu.make_async_copy(ref, ref, send.at[stage]).wait()

    load_points = pltpu.make_async_copy(points, cols.at[zh, x, zl], load.at[0])
    load_targets = pltpu.make_async_copy(targets, turned, load.at[1])
    load_points.start()
    load_targets.start()
    barrier = pltpu.get_barrier_semaphore()
    greeted = 0
    for peers in (z_peers, x_peers, y_peers):
        for device in peers():
            pl.semaphore_signal(barrier, inc=1, device_id=device, device_id_type=MESH)
            greeted += 1

    def block_of(d, at_x):
        other = (z + d) % Z
        return cols.at[other // ZL, at_x, other % ZL]

    def to_z(d, src, dst, stage):
        other = (z + d) % Z
        push(src, dst, stage, (x, other % ZL, y, c, other // ZL))

    def to_x(step, block, stage):
        push(block, block, stage, ((x + step) % X, zl, y, c, zh))

    def relayed(d):
        return 1 if d % 2 == 0 else 3

    def along_x(d):
        block = block_of(d, x)
        to_x(relayed(d), block, 20 + d)
        to_x(4 - relayed(d), block, 3)

    def relay(d):
        arrived(rows.at[:, 0], 20 + d)
        to_x(relayed(d), block_of(d, (x + 4 - relayed(d)) % X), 28)

    own_block = cols.at[zh, x, zl]
    load_points.wait()
    pl.semaphore_wait(barrier, greeted)
    to_z(4, own_block.at[1 - zh], own_block.at[1 - zh], 0)
    for d in (1, 7):
        to_z(d, own_block, own_block, 11 + (Z - d))
    along_x(0)
    for d in (2, 6, 3, 5):
        to_z(d, own_block, own_block, 11 + (Z - d))
    to_z(4, own_block.at[zh], own_block.at[zh], 11 + 4)
    for device in y_peers():
        push(own_block.at[zh], rows.at[zh, mine], 5, device)
    rows[zh, mine] = cols[zh, x, zl, zh]

    load_targets.wait()
    halves = swap_blocks(jnp.concatenate([turned[...], turned[...]], axis=1))
    b_own = jnp.where(zh == 0, halves[0:4], halves[4:8])
    vb[me] = b_own
    bi[mine] = b_own
    for device in z_peers():
        push(vb.at[me], vb.at[me], 1, device)
    for device in y_peers():
        push(bi.at[mine], bi.at[mine], 2, device)

    for d in (1, 7):
        arrived(rows.at[:, 0], 11 + d)
        along_x(d)
    relay(0)
    for d in (2, 6):
        arrived(rows.at[:, 0], 11 + d)
        along_x(d)
    arrived(rows.at[0, 0], 0)
    for device in y_peers():
        push(cols.at[1 - zh, x, zl, zh], rows.at[1 - zh, mine], 5, device)
    rows[1 - zh, mine] = cols[1 - zh, x, zl, zh]
    relay(1)
    relay(7)
    for d in (3, 5):
        arrived(rows.at[:, 0], 11 + d)
        along_x(d)
    relay(2)
    relay(6)
    arrived(rows.at[0, 0], 11 + 4)
    along_x(4)
    arrived(vb.at[0:7], 1)
    for device in x_peers():
        push(vb.at[pl.ds(x * Z, Z)], vb.at[pl.ds(x * Z, Z)], 4, device)
    relay(3)
    relay(5)
    relay(4)
    arrived(rows.at[:, 0:15], 5)

    scale = 0.5 / F * math.log2(math.e)
    row_points = jnp.concatenate(
        [rows[0].reshape(NY * HALF, 128), rows[1].reshape(NY * HALF, 128)], axis=1
    )
    wide = row_points.astype(F32)
    squares = wide * wide
    high = squares.astype(BF16)
    low = (squares - high.astype(F32)).astype(BF16)
    ones = jnp.ones((8, F), BF16)
    contract = (((1,), (1,)), ((), ()))
    row_norms = (
        lax.dot_general(ones, high, contract, preferred_element_type=F32)
        + lax.dot_general(ones, low, contract, preferred_element_type=F32)
    )[0:1] * scale

    for d in range(X):
        if d == 1:
            arrived(rows.at[:, 0:8], 3)
            arrived(rows.at[:, 0:8], 28)
        part = (x + d) % X
        col_points = jnp.concatenate(
            [cols[0, part].reshape(256, 128), cols[1, part].reshape(256, 128)], axis=1
        )
        wide = col_points.astype(F32)
        col_norms = jnp.sum(wide * wide, axis=1, keepdims=True) * scale
        inner = lax.dot_general(col_points, row_points, contract, preferred_element_type=F32)
        kmat[part] = jnp.exp2(
            (2.0 * scale) * inner - (row_norms + col_norms)
        ).astype(BF16)

    arrived(vb.at[0:24], 4)

    def partial_product(slots):
        wide = [
            swap_blocks(jnp.concatenate(slots[4 * j : 4 * j + 4], axis=0)).astype(BF16)
            for j in range(NXZ // 4)
        ]
        vector = jnp.concatenate(wide, axis=1)
        return jnp.dot(vector, kmat[...].reshape(NXZ * HALF, NY * HALF), preferred_element_type=F32)

    def to_owners(product, weights, ys, yr, stage):
        blocks = []
        for j in range(NY // 4):
            block = swap_blocks(product[:, 128 * j : 128 * j + 128])
            blocks += [block[4 * s : 4 * s + 4] for s in range(4)]
        share = group_sums(tree_sum([w * b for w, b in zip(weights, blocks)]))
        for t in range(NY):
            ys[t] = jnp.concatenate([blocks[t], share], axis=0)
        for device in y_peers():
            push(ys.at[device[2] * C + device[3]], yr.at[mine], stage, device)
        yr[mine] = ys[mine]
        arrived(yr.at[0:15], stage)
        return tree_sum([yr[t] for t in range(NY)])

    arrived(bi.at[0:15], 2)
    b_rows = [bi[t] for t in range(NY)]
    b_cols = [vb[s] for s in range(NXZ)]
    total = to_owners(partial_product(b_cols), b_rows, ys1, yr1, 6)
    bb_here = group_sums(tree_sum([b * b for b in b_rows]))
    w_own = total[0:4] + 0.1 * b_own
    vw[me] = jnp.concatenate([w_own, paired(total[4:8], bb_here)], axis=0)
    wi[mine] = w_own
    for device in xz_peers():
        push(vw.at[me], vw.at[me], 7, device)
    for device in y_peers():
        push(wi.at[mine], wi.at[mine], 8, device)
    arrived(vw.at[0:31], 7)
    bkb, bb = unpaired(tree_sum([vw[s, 4:8] for s in range(NXZ)]))
    alpha = bb / (bkb + 0.1 * bb)

    r_cols = [b_cols[s] - alpha * vw[s, 0:4] for s in range(NXZ)]
    product = partial_product(r_cols)
    arrived(wi.at[0:15], 8)
    r_rows = [b_rows[t] - alpha * wi[t] for t in range(NY)]
    rr_here = group_sums(tree_sum([r * r for r in r_rows]))
    total = to_owners(product, r_rows, ys2, yr2, 9)
    r_own = b_own - alpha * w_own
    u_own = total[0:4] + 0.1 * r_own
    sums[me] = paired(total[4:8], rr_here)
    for device in xz_peers():
        push(sums.at[me], sums.at[me], 10, device)
    vu[zh] = u_own
    to_z(4, vu.at[zh], vu.at[zh], 9 + 20)
    arrived(sums.at[0:31], 10)
    rkr, rr = unpaired(tree_sum([sums[s] for s in range(NXZ)]))
    ratio = rr / bb
    alpha_next = rr / (rkr + 0.1 * rr - ratio * rr / alpha)

    def result(halves, out):
        packed = jnp.concatenate([*halves, jnp.zeros((8, 128), F32)], axis=0)
        out[...] = swap_blocks(packed)[:, 0:64]

    arrived(vu.at[0], 29)
    solutions, residuals = [], []
    for h in range(2):
        b, w, u = vb[own + h], vw[own + h, 0:4], vu[h]
        r = b - alpha * w
        solutions.append(alpha * b + alpha_next * (r + ratio * b))
        residuals.append(r - alpha_next * (u + ratio * w))
    result(solutions, results.at[0])
    result(residuals, results.at[1])

    for ref, stage in pending:
        sent(ref, stage)


def local(points, targets):
    anywhere = pl.BlockSpec(memory_space=pl.ANY)
    message = lambda n, rows=8: pltpu.VMEM((n, rows, 128), F32)
    results = pl.pallas_call(
        kernel,
        out_shape=pltpu.VMEM((2, R, 2 * HALF), F32),
        in_specs=[anywhere, anywhere],
        out_specs=pl.BlockSpec(memory_space=pltpu.VMEM),
        scratch_shapes=[
            pltpu.VMEM((R, 2 * HALF), F32),
            pltpu.VMEM((2, X, ZL, ZH, HALF, 128), BF16),
            pltpu.VMEM((2, NY, HALF, 128), BF16),
            pltpu.VMEM((X, Z * HALF, NY * HALF), BF16),
            message(NXZ, 4), message(NXZ), message(ZH, 4), message(NXZ, 4),
            message(NY, 4), message(NY, 4),
            message(NY), message(NY), message(NY), message(NY),
            pltpu.SemaphoreType.DMA((2,)),
            pltpu.SemaphoreType.DMA((30,)),
            pltpu.SemaphoreType.DMA((30,)),
        ],
        compiler_params=pltpu.CompilerParams(collective_id=0, has_side_effects=True),
    )(points.reshape(2, HALF, 128), targets.T)
    return results[0].T, results[1].T


def solution(mesh):
    torus = Mesh(mesh.devices.reshape(X, ZL, Y, C, ZH), AXES)
    in_specs = (P(GX_GY, "af"), P(GX_GY, None))
    out_specs = (P(GX_GY, None), P(GX_GY, None))
    return jax.shard_map(local, mesh=torus, in_specs=in_specs, out_specs=out_specs, check_vma=False)
```

```python
import math

import jax
import jax.numpy as jnp
from jax import lax
from jax.experimental import pallas as pl
from jax.experimental.pallas import tpu as pltpu
from jax.sharding import Mesh
from jax.sharding import PartitionSpec as P

AXES = ("gx_0", "gx_1", "gy_0", "gy_1", "af")
GX_GY = ("gx_0", "gx_1", "gy_0", "gy_1")
MESH = pl.DeviceIdType.MESH
X, ZL, Y, C, ZH = 4, 4, 8, 2, 2
Z = ZL * ZH
NXZ, NY = X * Z, Y * C
HALF, F, R = 32, 256, 16
F32, BF16 = jnp.float32, jnp.bfloat16


def swap_blocks(tile):
    rows = lax.broadcasted_iota(jnp.int32, (16, 128), 0) // 4
    lanes = lax.broadcasted_iota(jnp.int32, (16, 128), 1) // 32
    shift = (rows - lanes) & 3
    out = tile
    for d in range(1, 4):
        moved = pltpu.roll(pltpu.roll(tile, 128 - 32 * d, 1), 4 * d, 0)
        out = jnp.where(shift == d, moved, out)
    return out


def group_sums(packed):
    group = lax.broadcasted_iota(jnp.int32, (4, 128), 1) // 32
    spread = jnp.concatenate([jnp.where(group == g, packed, 0.0) for g in range(4)], axis=0)
    sums = jnp.sum(spread, axis=1, keepdims=True)
    out = jnp.broadcast_to(sums[12:16], (4, 128))
    for g in range(3):
        out = jnp.where(group == g, sums[4 * g : 4 * g + 4], out)
    return out


def low_lanes():
    return (lax.broadcasted_iota(jnp.int32, (4, 128), 1) & 31) < 16


def paired(first, second):
    return jnp.where(low_lanes(), first, second)


def unpaired(both):
    low = low_lanes()
    return (
        jnp.where(low, both, pltpu.roll(both, 16, 1)),
        jnp.where(low, pltpu.roll(both, 112, 1), both),
    )


def tree_sum(terms):
    while len(terms) > 1:
        terms = [sum(terms[i : i + 2][1:], terms[i]) for i in range(0, len(terms), 2)]
    return terms[0]


def kernel(
    points, targets, results,
    turned, cols, rows, kmat, vb, vw, vu, sums, bi, wi, ys1, yr1, ys2, yr2, load, send, recv,
):
    x, zl, y, c, zh = (lax.axis_index(a) for a in AXES)
    z = zh * ZL + zl
    me = (x * ZL + zl) * ZH + zh
    mine = y * C + c
    own = (x * ZL + zl) * ZH

    def z_peers():
        for d in (4, 3, 5, 2, 6, 1, 7):
            other = (z + d) % Z
            yield (x, other % ZL, y, c, other // ZL)

    def x_peers():
        for d in (2, 1, 3):
            yield ((x + d) % X, zl, y, c, zh)

    def xz_peers():
        for dz in (4, 3, 5, 2, 6, 1, 7, 0):
            for dx in (2, 1, 3, 0):
                if dz or dx:
                    other = (z + dz) % Z
                    yield ((x + dx) % X, other % ZL, y, c, other // ZL)

    def y_peers():
        for d in (4, 3, 5, 2, 6, 1, 7, 0):
            for e in (1, 0):
                if d or e:
                    yield (x, zl, (y + d) % Y, (c + e) % C, zh)

    def push(src, dst, stage, device):
        pltpu.make_async_remote_copy(
            src_ref=src, dst_ref=dst, send_sem=send.at[stage], recv_sem=recv.at[stage],
            device_id=device, device_id_type=MESH,
        ).start()

    pending = []

    def arrived(ref, stage):
        pltpu.make_async_copy(ref, ref, recv.at[stage]).wait()
        pending.append((ref, stage))

    def sent(ref, stage):
        pltpu.make_async_copy(ref, ref, send.at[stage]).wait()

    load_points = pltpu.make_async_copy(points, cols.at[zh, x, zl], load.at[0])
    load_targets = pltpu.make_async_copy(targets, turned, load.at[1])
    load_points.start()
    load_targets.start()
    barrier = pltpu.get_barrier_semaphore()
    greeted = 0
    for peers in (z_peers, x_peers, y_peers):
        for device in peers():
            pl.semaphore_signal(barrier, inc=1, device_id=device, device_id_type=MESH)
            greeted += 1

    def block_of(d, at_x):
        other = (z + d) % Z
        return cols.at[other // ZL, at_x, other % ZL]

    def to_z(d, src, dst, stage):
        other = (z + d) % Z
        push(src, dst, stage, (x, other % ZL, y, c, other // ZL))

    def to_x(step, block, stage):
        push(block, block, stage, ((x + step) % X, zl, y, c, zh))

    def along_x(d):
        block = block_of(d, x)
        for step in (2, 1, 3):
            to_x(step, block, 3)

    own_block = cols.at[zh, x, zl]
    load_points.wait()
    pl.semaphore_wait(barrier, greeted)
    to_z(4, own_block.at[1 - zh], own_block.at[1 - zh], 0)
    for d in (1, 7):
        to_z(d, own_block, own_block, 11 + (Z - d))
    along_x(0)
    for d in (2, 6, 3, 5):
        to_z(d, own_block, own_block, 11 + (Z - d))
    to_z(4, own_block.at[zh], own_block.at[zh], 11 + 4)
    for device in y_peers():
        push(own_block.at[zh], rows.at[zh, mine], 5, device)
    rows[zh, mine] = cols[zh, x, zl, zh]

    load_targets.wait()
    halves = swap_blocks(jnp.concatenate([turned[...], turned[...]], axis=1))
    b_own = jnp.where(zh == 0, halves[0:4], halves[4:8])
    vb[me] = b_own
    bi[mine] = b_own
    for device in z_peers():
        push(vb.at[me], vb.at[me], 1, device)
    for device in y_peers():
        push(bi.at[mine], bi.at[mine], 2, device)

    for d in (1, 7):
        arrived(rows.at[:, 0], 11 + d)
        along_x(d)
    for d in (2, 6):
        arrived(rows.at[:, 0], 11 + d)
        along_x(d)
    arrived(rows.at[0, 0], 0)
    for device in y_peers():
        push(cols.at[1 - zh, x, zl, zh], rows.at[1 - zh, mine], 5, device)
    rows[1 - zh, mine] = cols[1 - zh, x, zl, zh]
    for d in (3, 5):
        arrived(rows.at[:, 0], 11 + d)
        along_x(d)
    arrived(rows.at[0, 0], 11 + 4)
    along_x(4)
    arrived(vb.at[0:7], 1)
    for device in x_peers():
        push(vb.at[pl.ds(x * Z, Z)], vb.at[pl.ds(x * Z, Z)], 4, device)
    arrived(rows.at[:, 0:15], 5)

    scale = 0.5 / F * math.log2(math.e)
    row_points = jnp.concatenate(
        [rows[0].reshape(NY * HALF, 128), rows[1].reshape(NY * HALF, 128)], axis=1
    )
    wide = row_points.astype(F32)
    squares = wide * wide
    high = squares.astype(BF16)
    low = (squares - high.astype(F32)).astype(BF16)
    ones = jnp.ones((8, F), BF16)
    contract = (((1,), (1,)), ((), ()))
    row_norms = (
        lax.dot_general(ones, high, contract, preferred_element_type=F32)
        + lax.dot_general(ones, low, contract, preferred_element_type=F32)
    )[0:1] * scale

    for d in range(X):
        if d == 1:
            arrived(cols.at[:, 0:3], 3)
        part = (x + d) % X
        col_points = jnp.concatenate(
            [cols[0, part].reshape(256, 128), cols[1, part].reshape(256, 128)], axis=1
        )
        wide = col_points.astype(F32)
        col_norms = jnp.sum(wide * wide, axis=1, keepdims=True) * scale
        inner = lax.dot_general(col_points, row_points, contract, preferred_element_type=F32)
        kmat[part] = jnp.exp2(
            (2.0 * scale) * inner - (row_norms + col_norms)
        ).astype(BF16)

    arrived(vb.at[0:24], 4)

    def partial_product(slots):
        wide = [
            swap_blocks(jnp.concatenate(slots[4 * j : 4 * j + 4], axis=0)).astype(BF16)
            for j in range(NXZ // 4)
        ]
        vector = jnp.concatenate(wide, axis=1)
        return jnp.dot(vector, kmat[...].reshape(NXZ * HALF, NY * HALF), preferred_element_type=F32)

    def to_owners(product, weights, ys, yr, stage):
        blocks = []
        for j in range(NY // 4):
            block = swap_blocks(product[:, 128 * j : 128 * j + 128])
            blocks += [block[4 * s : 4 * s + 4] for s in range(4)]
        share = group_sums(tree_sum([w * b for w, b in zip(weights, blocks)]))
        for t in range(NY):
            ys[t] = jnp.concatenate([blocks[t], share], axis=0)
        for device in y_peers():
            push(ys.at[device[2] * C + device[3]], yr.at[mine], stage, device)
        yr[mine] = ys[mine]
        arrived(yr.at[0:15], stage)
        return tree_sum([yr[t] for t in range(NY)])

    arrived(bi.at[0:15], 2)
    b_rows = [bi[t] for t in range(NY)]
    b_cols = [vb[s] for s in range(NXZ)]
    total = to_owners(partial_product(b_cols), b_rows, ys1, yr1, 6)
    bb_here = group_sums(tree_sum([b * b for b in b_rows]))
    w_own = total[0:4] + 0.1 * b_own
    vw[me] = jnp.concatenate([w_own, paired(total[4:8], bb_here)], axis=0)
    wi[mine] = w_own
    for device in xz_peers():
        push(vw.at[me], vw.at[me], 7, device)
    for device in y_peers():
        push(wi.at[mine], wi.at[mine], 8, device)
    arrived(vw.at[0:31], 7)
    bkb, bb = unpaired(tree_sum([vw[s, 4:8] for s in range(NXZ)]))
    alpha = bb / (bkb + 0.1 * bb)

    r_cols = [b_cols[s] - alpha * vw[s, 0:4] for s in range(NXZ)]
    product = partial_product(r_cols)
    arrived(wi.at[0:15], 8)
    r_rows = [b_rows[t] - alpha * wi[t] for t in range(NY)]
    rr_here = group_sums(tree_sum([r * r for r in r_rows]))
    total = to_owners(product, r_rows, ys2, yr2, 9)
    r_own = b_own - alpha * w_own
    u_own = total[0:4] + 0.1 * r_own
    sums[me] = paired(total[4:8], rr_here)
    for device in xz_peers():
        push(sums.at[me], sums.at[me], 10, device)
    vu[zh] = u_own
    to_z(4, vu.at[zh], vu.at[zh], 19)
    arrived(sums.at[0:31], 10)
    rkr, rr = unpaired(tree_sum([sums[s] for s in range(NXZ)]))
    ratio = rr / bb
    alpha_next = rr / (rkr + 0.1 * rr - ratio * rr / alpha)

    def result(halves, out):
        packed = jnp.concatenate([*halves, jnp.zeros((8, 128), F32)], axis=0)
        out[...] = swap_blocks(packed)[:, 0:64]

    arrived(vu.at[0], 19)
    solutions, residuals = [], []
    for h in range(2):
        b, w, u = vb[own + h], vw[own + h, 0:4], vu[h]
        r = b - alpha * w
        solutions.append(alpha * b + alpha_next * (r + ratio * b))
        residuals.append(r - alpha_next * (u + ratio * w))
    result(solutions, results.at[0])
    result(residuals, results.at[1])

    for ref, stage in pending:
        sent(ref, stage)


def local(points, targets):
    anywhere = pl.BlockSpec(memory_space=pl.ANY)
    message = lambda n, rows=8: pltpu.VMEM((n, rows, 128), F32)
    results = pl.pallas_call(
        kernel,
        out_shape=pltpu.VMEM((2, R, 2 * HALF), F32),
        in_specs=[anywhere, anywhere],
        out_specs=pl.BlockSpec(memory_space=pltpu.VMEM),
        scratch_shapes=[
            pltpu.VMEM((R, 2 * HALF), F32),
            pltpu.VMEM((2, X, ZL, ZH, HALF, 128), BF16),
            pltpu.VMEM((2, NY, HALF, 128), BF16),
            pltpu.VMEM((X, Z * HALF, NY * HALF), BF16),
            message(NXZ, 4), message(NXZ), message(ZH, 4), message(NXZ, 4),
            message(NY, 4), message(NY, 4),
            message(NY), message(NY), message(NY), message(NY),
            pltpu.SemaphoreType.DMA((2,)),
            pltpu.SemaphoreType.DMA((20,)),
            pltpu.SemaphoreType.DMA((20,)),
        ],
        compiler_params=pltpu.CompilerParams(collective_id=0, has_side_effects=True),
    )(points.reshape(2, HALF, 128), targets.T)
    return results[0].T, results[1].T


def solution(mesh):
    torus = Mesh(mesh.devices.reshape(X, ZL, Y, C, ZH), AXES)
    in_specs = (P(GX_GY, "af"), P(GX_GY, None))
    out_specs = (P(GX_GY, None), P(GX_GY, None))
    return jax.shard_map(local, mesh=torus, in_specs=in_specs, out_specs=out_specs, check_vma=False)
```
